32 devices in a mesh: gx: 8 (over y, x, core), gy: 4 (over z).
Axes of the slice: x: 2, y: 2, z: 4, core: 2. Of those that a mesh axis runs over, the one named last changes fastest.
Arguments:
- right_side: float32 [1024, 2048], P('gx', 'gy'), may hold values from -6 to 6
- kappa_field: float32 [1024, 2048], P('gx', 'gy'), may hold values from 0.0001 to 0.01
- ice_blocks: int32 [128, 256], P('gx', 'gy'), may hold values 0 or 1
Outputs:
- solution_field: float32 [1024, 2048], P('gx', 'gy')
The draws below stay inside these ranges and needn't reach their ends.
All inputs are finite; a program needn't handle non-finite values. No bound on the sum of `ice_blocks` on one device may be relied on, other than what follows from the above.
Results may differ from the reference program's by a relative error of at most 0.0001.
Values sent between devices are 32-bit elements; how exact they have to be, the bound alone decides.
No kernel may reach another device: no remote copies, remote signals or barrier semaphores. Data moves between devices by JAX's collectives and lax.ppermute only.
A program may use at most 64 MiB of HBM per device.

```python
import math
import jax
import jax.numpy as jnp

BLOCK = 8
NU = 2
NC = 16
NX = 1024
NY = 2048


def set_ends(array, stream_key, smallest, largest):
    longest = array.shape.index(max(array.shape))
    spots = []
    for shift in (0, 1):
        where = [jax.random.randint(jax.random.fold_in(stream_key, axis), (), 0, length) for axis, length in enumerate(array.shape)]
        where[longest] = (where[longest] + shift) % array.shape[longest]
        spots.append(tuple(where))
    return array.at[spots[0]].set(smallest).at[spots[1]].set(largest)


def block_scale(own_key, dims, shards, least, largest):
    gain = 1.0
    for dim, shards_of in shards:
        draws = jax.random.uniform(jax.random.fold_in(jax.random.fold_in(own_key, 6), dim), (shards_of,), jnp.float32, least / len(shards), largest / len(shards))
        gain = gain * jnp.repeat(jnp.exp(draws), dims[dim] // shards_of).reshape((-1,) + (1,) * (len(dims) - 1 - dim))
    return gain


def bell_draw(rng, dims, spread, limit, split=(), kind=jnp.bfloat16):
    array = jax.random.normal(rng, dims, jnp.float32) * spread
    if len(split) > 0:
        array = block_scale(rng, dims, split, -0.22, 0.18) * array
    return jnp.clip(array, min=-limit, max=limit).astype(kind)


def setup_inputs(seed: int = 0) -> dict:
    streams_of = jax.random.split(jax.random.key(seed), 4)
    right_side = bell_draw(streams_of[0], (NX, NY), 1.0, 6.0, ((0, 8), (1, 4)), jnp.float32)
    kappa_field = jnp.clip(jnp.exp(math.log(0.01) - 4.6051702 * jax.random.uniform(streams_of[1], (NX, NY), jnp.float32) ** block_scale(streams_of[1], (NX, NY), ((0, 8), (1, 4)), -0.2, 0.2)), 0.0001, 0.01)
    ice_blocks = set_ends((jax.random.randint(streams_of[2], (NX // BLOCK, NY // BLOCK), 0, 4) < 3).astype(jnp.int32), jax.random.fold_in(streams_of[2], 1), 0, 1)
    return dict(right_side=right_side, kappa_field=kappa_field, ice_blocks=ice_blocks)


damping = 0.8


def apply_operator(padded, reaction, stiffness):
    middle = padded[1:-1, 1:-1]
    beside = padded[2:, 1:-1] + padded[:-2, 1:-1]
    beside = beside + padded[1:-1, 2:] + padded[1:-1, :-2]
    return reaction * middle + stiffness * (4.0 * middle - beside)


def jacobi_step(padded, source, reaction, stiffness):
    middle = padded[1:-1, 1:-1]
    applied = apply_operator(padded, reaction, stiffness)
    return middle + damping * (source - applied) / (reaction + 4.0 * stiffness)


def restrict(field):
    height, width = field.shape
    return field.reshape(height // 2, 2, width // 2, 2).mean(axis=(1, 3))


def prolong(field):
    return jnp.repeat(jnp.repeat(field, 2, axis=0), 2, axis=1)


def reference(right_side, kappa_field, ice_blocks):
    ice = jnp.repeat(jnp.repeat(ice_blocks, BLOCK, axis=0), BLOCK, axis=1).astype(jnp.float32)
    reaction = kappa_field * (1.0 + 3.0 * (1.0 - ice))
    source = right_side
    stored = []
    for level in range(3):
        stiffness = 0.25 ** level
        field = jnp.zeros_like(source)
        for sweep in range(NU):
            field = jacobi_step(jnp.pad(field, 1), source, reaction, stiffness)
        stored.append((field, source, reaction))
        residual = source - apply_operator(jnp.pad(field, 1), reaction, stiffness)
        source = restrict(residual)
        reaction = restrict(reaction)
    field = jnp.zeros_like(source)
    for sweep in range(NC):
        field = jacobi_step(jnp.pad(field, 1), source, reaction, 0.25 ** 3)
    for level in (2, 1, 0):
        stiffness = 0.25 ** level
        before, source, reaction = stored[level]
        field = before + prolong(field)
        for sweep in range(NU):
            field = jacobi_step(jnp.pad(field, 1), source, reaction, stiffness)
    return field
```

```python
import functools

import jax
import jax.numpy as jnp
from jax import lax
from jax.experimental import pallas as pl
from jax.experimental.pallas import tpu as pltpu
from jax.sharding import PartitionSpec as P

BLOCK = 8
NC = 16
LANES = 128
ROWS = 32
NEAR = 128
FAR = 32
damping = 0.8

f32 = jnp.float32
HIGHEST = lax.Precision.HIGHEST


def roll(value, shift, axis):
    return pltpu.roll(value, shift % value.shape[axis], axis)


def around(value, step):
    rows = roll(value, 1, 0) + roll(value, -1, 0)
    return rows + (roll(value, step, 1) + roll(value, -step, 1))


def iota(shape, axis):
    return lax.broadcasted_iota(jnp.int32, shape, axis)


def ones_where(condition):
    return jnp.where(condition, 1.0, 0.0).astype(f32)


def pack_near_far(tiles, near_tile, far_tile, far_lane):
    far = tiles[:, far_tile * LANES : (far_tile + 1) * LANES]
    near = tiles[:, near_tile * LANES : (near_tile + 1) * LANES]
    count = LANES // FAR
    group = tiles.shape[0] // count
    lane = iota((group, LANES), 1) // FAR
    packed = jnp.zeros((group, LANES), f32)
    for g in range(count):
        moved = roll(far[g * group : (g + 1) * group], FAR * g - far_lane, 1)
        packed = jnp.where(lane == g, moved, packed)
    return near, packed


def edges_kernel(right_ref, kappa_ref, ice_ref, reaction_ref, even_ref, odd_ref):
    height, width = right_ref.shape
    blocks = ice_ref.shape
    ice = ice_ref[...].astype(f32)
    spread = ones_where(iota((blocks[1], width), 1) // BLOCK == iota((blocks[1], width), 0))
    repeat = ones_where(iota((height, blocks[0]), 0) // BLOCK == iota((height, blocks[0]), 1))
    ice = jnp.dot(ice, spread, preferred_element_type=f32)
    ice = jnp.dot(repeat, ice, preferred_element_type=f32)
    reaction = kappa_ref[...] * (1.0 + 3.0 * (1.0 - ice))
    reaction_ref[...] = reaction
    tiles = width // LANES
    even = lax.rem(lax.axis_index("gy"), 2) == 0
    size = height + height * FAR // LANES
    for k, field in enumerate((right_ref[...], reaction)):
        to_right = pack_near_far(field, tiles - 1, tiles - 2, LANES - FAR)
        to_left = pack_near_far(field, 0, 1, 0)
        start = k * size
        for a, b in zip(to_right, to_left):
            stop = start + a.shape[0]
            even_ref[start:stop, :] = jnp.where(even, a, b)
            odd_ref[start:stop, :] = jnp.where(even, b, a)
            start = stop


def widen_columns(own, even_msg, odd_msg, even, rows):
    height, width = own.shape
    from_right = jnp.where(even, even_msg, odd_msg)
    from_left = jnp.where(even, odd_msg, even_msg)
    count = LANES // FAR
    group = height // count
    far_right = from_right[height:]
    far_left = from_left[height:]
    pieces = []
    lane = iota((group, LANES), 1)
    for g in range(count):
        if g * group >= rows[1] or (g + 1) * group <= rows[0]:
            continue
        piece = jnp.where(lane < FAR, roll(far_right, -FAR * g, 1), 0.0)
        piece = jnp.where(lane >= LANES - FAR, roll(far_left, LANES - FAR - FAR * g, 1), piece)
        pieces.append(piece)
    far = jnp.concatenate(pieces, axis=0) if len(pieces) > 1 else pieces[0]
    near_left = from_left[rows[0] : rows[1]]
    near_right = from_right[rows[0] : rows[1]]
    return jnp.concatenate([near_left, own[rows[0] : rows[1]], near_right, far], axis=1)


def rows_kernel(right_ref, reaction_ref, even_ref, odd_ref, even_out, odd_out):
    height = right_ref.shape[0]
    even_column = lax.rem(lax.axis_index("gy"), 2) == 0
    even_row = lax.rem(lax.axis_index("gx"), 2) == 0
    size = even_ref.shape[0] // 2
    for k, ref in enumerate((right_ref, reaction_ref)):
        a = even_ref[k * size : (k + 1) * size]
        b = odd_ref[k * size : (k + 1) * size]
        up = widen_columns(ref[...], a, b, even_column, (0, ROWS))
        down = widen_columns(ref[...], a, b, even_column, (height - ROWS, height))
        even_out[k * ROWS : (k + 1) * ROWS] = jnp.where(even_row, down, up)
        odd_out[k * ROWS : (k + 1) * ROWS] = jnp.where(even_row, up, down)


def pair_rows(value, scratch):
    rows, width = value.shape
    pieces = []
    for j in range(width // LANES):
        scratch[j, :rows] = value[:, j * LANES : (j + 1) * LANES]
        first = scratch[j, pl.ds(0, rows // 2, stride=2), :]
        second = scratch[j, pl.ds(1, rows // 2, stride=2), :]
        pieces.append(first + second)
    return jnp.concatenate(pieces, axis=1)


def pair_lanes(value, step):
    lane = iota(value.shape, 1)
    other = jnp.where((lane // step) % 2 == 0, roll(value, -step, 1), roll(value, step, 1))
    return value + other


def double_rows(value, scratch):
    rows, width = value.shape
    pieces = []
    for j in range(width // LANES):
        piece = value[:, j * LANES : (j + 1) * LANES]
        scratch[j, pl.ds(0, rows, stride=2), :] = piece
        scratch[j, pl.ds(1, rows, stride=2), :] = piece
        pieces.append(scratch[j, : 2 * rows])
    return jnp.concatenate(pieces, axis=1)


def keep_post(value, top, rows, ref):
    value = value[top : top + rows]
    width = value.shape[1] - 3 * LANES
    lane = iota((rows, LANES), 1)
    left = value[:, :LANES]
    right = value[:, LANES + width : 2 * LANES + width]
    ref[:, :width] = value[:, LANES : LANES + width]
    ref[:, width:] = jnp.where(lane < LANES // 2, right, left)


def down_kernel(height, width, grid_rows, grid_cols, *refs):
    right_ref, reaction_ref, even_ref, odd_ref, even_rows, odd_rows = refs[:6]
    outs = refs[6:15]
    own_out, even_out, odd_out = refs[15:18]
    scratch = refs[18]
    even_column = lax.rem(lax.axis_index("gy"), 2) == 0
    even_row = lax.rem(lax.axis_index("gx"), 2) == 0
    size = even_ref.shape[0] // 2
    fields = []
    for k, ref in enumerate((right_ref, reaction_ref)):
        a = even_ref[k * size : (k + 1) * size]
        b = odd_ref[k * size : (k + 1) * size]
        own = widen_columns(ref[...], a, b, even_column, (0, height))
        a = even_rows[k * ROWS : (k + 1) * ROWS]
        b = odd_rows[k * ROWS : (k + 1) * ROWS]
        top = jnp.where(even_row, b, a)
        bottom = jnp.where(even_row, a, b)
        fields.append(jnp.concatenate([top, own, bottom], axis=0))
    source, reaction = fields
    total = source.shape[1]
    first_row = lax.axis_index("gx") * height - ROWS
    first_col = lax.axis_index("gy") * width
    col = iota((1, total), 1)
    col = jnp.where(col >= total - FAR, col - total, col) - NEAR + first_col
    col_in = ones_where((col >= 0) & (col < grid_cols))
    margin = ROWS
    for level in range(3):
        rows = source.shape[0]
        row = first_row + iota((rows, 1), 0) * 2**level
        inside = ones_where((row >= 0) & (row < grid_rows)) * col_in
        stiffness = 0.25**level
        step = 2**level
        diagonal = reaction + 4.0 * stiffness
        gain = inside * (damping / diagonal)
        field = gain * source
        field = gain * ((2.0 - damping) * source + stiffness * around(field, step))
        keep = min(margin, 8)
        kept = rows - 2 * (margin - keep)
        for value, ref in zip((field, source, gain), outs[3 * level : 3 * level + 3]):
            keep_post(value, margin - keep, kept, ref)
        residual = source - diagonal * field + stiffness * around(field, step)
        source = pair_rows(residual, scratch)
        reaction = pair_rows(reaction, scratch)
        margin //= 2
        if level < 2:
            source = 0.25 * pair_lanes(source, step)
            reaction = 0.25 * pair_lanes(reaction, step)
    cell = iota((total, LANES), 0)
    step = 4
    target = jnp.where(cell >= total - FAR, cell - total + 8 * LANES, cell) // 8
    valid = (cell % step == 0) & ((cell < total - LANES + FAR) | (cell >= total - FAR))
    gather = ones_where(valid & (target == iota((total, LANES), 1)))
    coarse_rows = source.shape[0]
    for k, value in enumerate((source, reaction)):
        compact = 0.25 * jnp.dot(value, gather, precision=HIGHEST, preferred_element_type=f32)
        own_out[k * coarse_rows : (k + 1) * coarse_rows] = compact
        half = height // 8
        to_next = compact[margin - 1 : margin - 1 + half]
        to_last = compact[margin + 1 : margin + 1 + half]
        even_out[k * half : (k + 1) * half] = jnp.where(even_row, to_next, to_last)
        odd_out[k * half : (k + 1) * half] = jnp.where(even_row, to_last, to_next)


def up_kernel(height, width, grid_rows, grid_cols, *refs):
    posts = refs[:9]
    own_ref, even_ref, odd_ref = refs[9:12]
    out_ref = refs[12]
    scratch, region = refs[13:15]
    even_row = lax.rem(lax.axis_index("gx"), 2) == 0
    half = height // 8
    coarse_rows = own_ref.shape[0] // 2
    margin = (coarse_rows - half) // 2
    lead = 8 + half
    rows = region.shape[1]
    region[...] = jnp.zeros_like(region)
    for k in range(2):
        a = even_ref[k * half : (k + 1) * half]
        b = odd_ref[k * half : (k + 1) * half]
        own = own_ref[k * coarse_rows : (k + 1) * coarse_rows]
        region[k, lead - 1 - half : lead - 1] = jnp.where(even_row, b, a)
        region[k, lead - 1 : lead + half + 1] = own[margin - 1 : margin + half + 1]
        region[k, lead + half + 1 : lead + 2 * half + 1] = jnp.where(even_row, a, b)
    stiffness = 0.25**3
    row = lax.axis_index("gx") * half - lead + iota((rows, LANES), 0)
    col = iota((rows, LANES), 1)
    col = jnp.where(col >= LANES - FAR // 8, col - LANES, col) - NEAR // 8
    col = col + lax.axis_index("gy") * (width // 8)
    inside = (row >= 0) & (row < grid_rows // 8) & (col >= 0) & (col < grid_cols // 8)
    gain = ones_where(inside) * (damping / (region[1] + 4.0 * stiffness))
    field = gain * region[0]
    constant = field
    gain = gain * stiffness
    for sweep in range(NC - 1):
        field = (1.0 - damping) * field + constant + gain * around(field, 1)
    field = field[lead - margin : lead - margin + coarse_rows]
    total = width + LANES
    position = iota((LANES, total), 1)
    position = jnp.where(position >= width + LANES // 2, position - total, position)
    source_lane = (position + NEAR) // 8
    expand = ones_where(source_lane == iota((LANES, total), 0))
    field = jnp.dot(field, expand, precision=HIGHEST, preferred_element_type=f32)
    for level in (2, 1, 0):
        before, source, gain = [ref[...] for ref in posts[3 * level : 3 * level + 3]]
        field = before + double_rows(field, scratch)
        stiffness = 0.25**level
        constant = gain * source
        gain = gain * stiffness
        for sweep in range(2):
            field = (1.0 - damping) * field + constant + gain * around(field, 2**level)
        if level > 0:
            field = field[4 : field.shape[0] - 4]
    out_ref[...] = field[8 : 8 + height, :width]


def swap_pairs(counts, axis):
    nx, ny = counts
    even, odd = [], []
    for i in range(nx):
        for j in range(ny):
            here = i * ny + j
            place = (i, j)[axis]
            last = counts[axis] - 1
            hop = ny if axis == 0 else 1
            even.append((here, here + hop * (1 - 2 * (place % 2))))
            if place in (0, last):
                other = (i * ny + (j ^ 1)) if axis == 0 else ((i ^ 1) * ny + j)
                odd.append((here, other))
            else:
                odd.append((here, here + hop * (2 * (place % 2) - 1)))
    return even, odd


def shape(*dims):
    return jax.ShapeDtypeStruct(dims, f32)


def per_device(counts, right_side, kappa_field, ice_blocks):
    height, width = right_side.shape
    grid_rows, grid_cols = height * counts[0], width * counts[1]
    axes = ("gx", "gy")
    row_even, row_odd = swap_pairs(counts, 0)
    col_even, col_odd = swap_pairs(counts, 1)
    packed = 2 * (height + height * FAR // LANES)
    reaction, even, odd = pl.pallas_call(
        edges_kernel,
        out_shape=(shape(height, width), shape(packed, LANES), shape(packed, LANES)),
        name="edges",
    )(right_side, kappa_field, ice_blocks)
    odd = lax.ppermute(odd, axes, col_odd)
    even = lax.ppermute(even, axes, col_even)
    total = width + 2 * NEAR + LANES
    even_rows, odd_rows = pl.pallas_call(
        rows_kernel,
        out_shape=(shape(2 * ROWS, total), shape(2 * ROWS, total)),
        name="rows",
    )(right_side, reaction, even, odd)
    odd_rows = lax.ppermute(odd_rows, axes, row_odd)
    even_rows = lax.ppermute(even_rows, axes, row_even)
    half = height // 8
    post_shapes = []
    for level in range(3):
        post_shapes += [shape((height >> level) + 16, width + LANES)] * 3
    coarse_rows = half + ROWS // 4
    outs = pl.pallas_call(
        functools.partial(down_kernel, height, width, grid_rows, grid_cols),
        out_shape=(*post_shapes, shape(2 * coarse_rows, LANES), shape(2 * half, LANES), shape(2 * half, LANES)),
        scratch_shapes=[pltpu.VMEM((total // LANES, height + 2 * ROWS, LANES), f32)],
        name="down",
    )(right_side, reaction, even, odd, even_rows, odd_rows)
    posts, own, even, odd = outs[:9], outs[9], outs[10], outs[11]
    odd = lax.ppermute(odd, axes, row_odd)
    even = lax.ppermute(even, axes, row_even)
    return pl.pallas_call(
        functools.partial(up_kernel, height, width, grid_rows, grid_cols),
        out_shape=shape(height, width),
        scratch_shapes=[
            pltpu.VMEM((width // LANES + 1, height + 16, LANES), f32),
            pltpu.VMEM((2, half * 3 + 16, LANES), f32),
        ],
        name="up",
    )(*posts, own, even, odd)


def solution(mesh):
    counts = (mesh.shape["gx"], mesh.shape["gy"])
    return jax.shard_map(
        functools.partial(per_device, counts),
        mesh=mesh,
        in_specs=(P("gx", "gy"),) * 3,
        out_specs=P("gx", "gy"),
        check_vma=False,
    )
```

```python
import functools

import jax
import jax.numpy as jnp
from jax import lax
from jax.experimental import pallas as pl
from jax.experimental.pallas import tpu as pltpu
from jax.sharding import PartitionSpec as P

BLOCK = 8
NC = 16
LANES = 128
ROWS = 32
NEAR = 128
FAR = 32
VMEM_BYTES = 12 * 2**20
damping = 0.8

f32 = jnp.float32
HIGHEST = lax.Precision.HIGHEST


def roll(value, shift, axis):
    return pltpu.roll(value, shift % value.shape[axis], axis)


def around(value, step):
    rows = roll(value, 1, 0) + roll(value, -1, 0)
    return rows + (roll(value, step, 1) + roll(value, -step, 1))


def iota(shape, axis):
    return lax.broadcasted_iota(jnp.int32, shape, axis)


def ones_where(condition):
    return jnp.where(condition, 1.0, 0.0).astype(f32)


def pack_near_far(tiles, near_tile, far_tile, far_lane):
    far = tiles[:, far_tile * LANES : (far_tile + 1) * LANES]
    near = tiles[:, near_tile * LANES : (near_tile + 1) * LANES]
    count = LANES // FAR
    group = tiles.shape[0] // count
    lane = iota((group, LANES), 1) // FAR
    packed = jnp.zeros((group, LANES), f32)
    for g in range(count):
        moved = roll(far[g * group : (g + 1) * group], FAR * g - far_lane, 1)
        packed = jnp.where(lane == g, moved, packed)
    return near, packed


def edges_kernel(*refs):
    ins, right_ref, reaction_ref, even_ref, odd_ref, rows_ref = refs[:3], *refs[3:8]
    kappa_ref, ice_ref, sems = refs[8:11]
    copies = []
    for k, (src, dst) in enumerate(zip(ins, (right_ref, kappa_ref, ice_ref))):
        copies.append(pltpu.make_async_copy(src, dst, sems.at[k]))
    for copy in copies:
        copy.start()
    height, width = right_ref.shape
    blocks = ice_ref.shape
    spread = ones_where(iota((blocks[1], width), 1) // BLOCK == iota((blocks[1], width), 0))
    repeat = ones_where(iota((height, blocks[0]), 0) // BLOCK == iota((height, blocks[0]), 1))
    for copy in copies:
        copy.wait()
    ice = ice_ref[...].astype(f32)
    ice = jnp.dot(ice, spread, preferred_element_type=f32)
    ice = jnp.dot(repeat, ice, preferred_element_type=f32)
    reaction = kappa_ref[...] * (1.0 + 3.0 * (1.0 - ice))
    reaction_ref[...] = reaction
    tiles = width // LANES
    even = lax.rem(lax.axis_index("gy"), 2) == 0
    even_row = lax.rem(lax.axis_index("gx"), 2) == 0
    size = height + height * FAR // LANES
    for k, field in enumerate((right_ref[...], reaction)):
        to_right = pack_near_far(field, tiles - 1, tiles - 2, LANES - FAR)
        to_left = pack_near_far(field, 0, 1, 0)
        start = k * size
        for a, b in zip(to_right, to_left):
            stop = start + a.shape[0]
            even_ref[start:stop, :] = jnp.where(even, a, b)
            odd_ref[start:stop, :] = jnp.where(even, b, a)
            start = stop
        rows_ref[k * ROWS : (k + 1) * ROWS] = jnp.where(even_row, field[:ROWS], field[height - ROWS :])


def widen_columns(own, even_msg, odd_msg, even, rows):
    height, width = own.shape
    from_right = jnp.where(even, even_msg, odd_msg)
    from_left = jnp.where(even, odd_msg, even_msg)
    count = LANES // FAR
    group = height // count
    far_right = from_right[height:]
    far_left = from_left[height:]
    pieces = []
    lane = iota((group, LANES), 1)
    for g in range(count):
        if g * group >= rows[1] or (g + 1) * group <= rows[0]:
            continue
        piece = jnp.where(lane < FAR, roll(far_right, -FAR * g, 1), 0.0)
        piece = jnp.where(lane >= LANES - FAR, roll(far_left, LANES - FAR - FAR * g, 1), piece)
        pieces.append(piece)
    far = jnp.concatenate(pieces, axis=0) if len(pieces) > 1 else pieces[0]
    near_left = from_left[rows[0] : rows[1]]
    near_right = from_right[rows[0] : rows[1]]
    return jnp.concatenate([near_left, own[rows[0] : rows[1]], near_right, far], axis=1)


def rows_kernel(right_ref, reaction_ref, even_ref, odd_ref, unread_ref, even_out, odd_out):
    height, width = right_ref.shape
    even_column = lax.rem(lax.axis_index("gy"), 2) == 0
    even_row = lax.rem(lax.axis_index("gx"), 2) == 0
    size = even_ref.shape[0] // 2
    far = []
    for k, ref in enumerate((right_ref, reaction_ref)):
        a = even_ref[k * size : (k + 1) * size]
        b = odd_ref[k * size : (k + 1) * size]
        up = widen_columns(ref[...], a, b, even_column, (0, ROWS))
        down = widen_columns(ref[...], a, b, even_column, (height - ROWS, height))
        even_out[k * ROWS : (k + 1) * ROWS] = jnp.where(even_row, down, up)
        odd = jnp.where(even_row, up, down)
        odd_out[:, 2 * k * LANES : (2 * k + 1) * LANES] = odd[:, :LANES]
        odd_out[:, (2 * k + 1) * LANES : (2 * k + 2) * LANES] = odd[:, width + LANES : width + 2 * LANES]
        far.append(odd[:, width + 2 * LANES :])
    lane = iota((ROWS, LANES), 1)
    odd_out[:, 4 * LANES :] = jnp.where((lane >= FAR) & (lane < LANES - FAR), roll(far[1], LANES // 2, 1), far[0])


def pair_rows(value, scratch):
    rows, width = value.shape
    pieces = []
    for j in range(width // LANES):
        scratch[j, :rows] = value[:, j * LANES : (j + 1) * LANES]
        first = scratch[j, pl.ds(0, rows // 2, stride=2), :]
        second = scratch[j, pl.ds(1, rows // 2, stride=2), :]
        pieces.append(first + second)
    return jnp.concatenate(pieces, axis=1)


def pair_lanes(value, step):
    lane = iota(value.shape, 1)
    other = jnp.where((lane // step) % 2 == 0, roll(value, -step, 1), roll(value, step, 1))
    return value + other


def double_rows(value, scratch):
    rows, width = value.shape
    pieces = []
    for j in range(width // LANES):
        piece = value[:, j * LANES : (j + 1) * LANES]
        scratch[j, pl.ds(0, rows, stride=2), :] = piece
        scratch[j, pl.ds(1, rows, stride=2), :] = piece
        pieces.append(scratch[j, : 2 * rows])
    return jnp.concatenate(pieces, axis=1)


def keep_post(value, top, rows, ref):
    value = value[top : top + rows]
    width = value.shape[1] - 3 * LANES
    lane = iota((rows, LANES), 1)
    left = value[:, :LANES]
    right = value[:, LANES + width : 2 * LANES + width]
    ref[:, :width] = value[:, LANES : LANES + width]
    ref[:, width:] = jnp.where(lane < LANES // 2, right, left)


def down_kernel(height, width, grid_rows, grid_cols, *refs):
    right_ref, reaction_ref, even_ref, odd_ref, even_rows, odd_rows, odd_corners = refs[:7]
    outs = refs[7:16]
    own_out, even_out, odd_out = refs[16:19]
    scratch = refs[19]
    even_column = lax.rem(lax.axis_index("gy"), 2) == 0
    even_row = lax.rem(lax.axis_index("gx"), 2) == 0
    size = even_ref.shape[0] // 2
    fields = []
    for k, ref in enumerate((right_ref, reaction_ref)):
        a = even_ref[k * size : (k + 1) * size]
        b = odd_ref[k * size : (k + 1) * size]
        own = widen_columns(ref[...], a, b, even_column, (0, height))
        a = even_rows[k * ROWS : (k + 1) * ROWS]
        far = odd_corners[:, 4 * LANES :]
        if k == 1:
            far = roll(far, LANES // 2, 1)
        b = jnp.concatenate(
            [
                odd_corners[:, 2 * k * LANES : (2 * k + 1) * LANES],
                odd_rows[k * ROWS : (k + 1) * ROWS],
                odd_corners[:, (2 * k + 1) * LANES : (2 * k + 2) * LANES],
                far,
            ],
            axis=1,
        )
        top = jnp.where(even_row, b, a)
        bottom = jnp.where(even_row, a, b)
        fields.append(jnp.concatenate([top, own, bottom], axis=0))
    source, reaction = fields
    total = source.shape[1]
    first_row = lax.axis_index("gx") * height - ROWS
    first_col = lax.axis_index("gy") * width
    col = iota((1, total), 1)
    col = jnp.where(col >= total - FAR, col - total, col) - NEAR + first_col
    col_in = ones_where((col >= 0) & (col < grid_cols))
    margin = ROWS
    for level in range(3):
        rows = source.shape[0]
        row = first_row + iota((rows, 1), 0) * 2**level
        inside = ones_where((row >= 0) & (row < grid_rows)) * col_in
        stiffness = 0.25**level
        step = 2**level
        diagonal = reaction + 4.0 * stiffness
        gain = inside * (damping / diagonal)
        field = gain * source
        field = gain * ((2.0 - damping) * source + stiffness * around(field, step))
        keep = min(margin, 8)
        kept = rows - 2 * (margin - keep)
        for value, ref in zip((field, source, gain), outs[3 * level : 3 * level + 3]):
            keep_post(value, margin - keep, kept, ref)
        residual = source - diagonal * field + stiffness * around(field, step)
        source = pair_rows(residual, scratch)
        reaction = pair_rows(reaction, scratch)
        margin //= 2
        if level < 2:
            source = 0.25 * pair_lanes(source, step)
            reaction = 0.25 * pair_lanes(reaction, step)
    cell = iota((total, LANES), 0)
    step = 4
    target = jnp.where(cell >= total - FAR, cell - total + 8 * LANES, cell) // 8
    valid = (cell % step == 0) & ((cell < total - LANES + FAR) | (cell >= total - FAR))
    gather = ones_where(valid & (target == iota((total, LANES), 1)))
    coarse_rows = source.shape[0]
    for k, value in enumerate((source, reaction)):
        compact = 0.25 * jnp.dot(value, gather, precision=HIGHEST, preferred_element_type=f32)
        own_out[k * coarse_rows : (k + 1) * coarse_rows] = compact
        half = height // 8
        to_next = compact[margin - 1 : margin - 1 + half]
        to_last = compact[margin + 1 : margin + 1 + half]
        even_out[k * half : (k + 1) * half] = jnp.where(even_row, to_next, to_last)
        odd_out[k * half : (k + 1) * half] = jnp.where(even_row, to_last, to_next)


def up_kernel(height, width, grid_rows, grid_cols, *refs):
    posts = refs[:9]
    own_ref, even_ref, odd_ref = refs[9:12]
    out_ref = refs[12]
    scratch, region = refs[13:15]
    even_row = lax.rem(lax.axis_index("gx"), 2) == 0
    half = height // 8
    coarse_rows = own_ref.shape[0] // 2
    margin = (coarse_rows - half) // 2
    lead = 8 + half
    rows = region.shape[1]
    region[...] = jnp.zeros_like(region)
    for k in range(2):
        a = even_ref[k * half : (k + 1) * half]
        b = odd_ref[k * half : (k + 1) * half]
        own = own_ref[k * coarse_rows : (k + 1) * coarse_rows]
        region[k, lead - 1 - half : lead - 1] = jnp.where(even_row, b, a)
        region[k, lead - 1 : lead + half + 1] = own[margin - 1 : margin + half + 1]
        region[k, lead + half + 1 : lead + 2 * half + 1] = jnp.where(even_row, a, b)
    stiffness = 0.25**3
    row = lax.axis_index("gx") * half - lead + iota((rows, LANES), 0)
    col = iota((rows, LANES), 1)
    col = jnp.where(col >= LANES - FAR // 8, col - LANES, col) - NEAR // 8
    col = col + lax.axis_index("gy") * (width // 8)
    inside = (row >= 0) & (row < grid_rows // 8) & (col >= 0) & (col < grid_cols // 8)
    gain = ones_where(inside) * (damping / (region[1] + 4.0 * stiffness))
    field = gain * region[0]
    constant = field
    gain = gain * stiffness
    for sweep in range(NC - 1):
        field = (1.0 - damping) * field + constant + gain * around(field, 1)
    field = field[lead - margin : lead - margin + coarse_rows]
    total = width + LANES
    position = iota((LANES, total), 1)
    position = jnp.where(position >= width + LANES // 2, position - total, position)
    source_lane = (position + NEAR) // 8
    expand = ones_where(source_lane == iota((LANES, total), 0))
    field = jnp.dot(field, expand, precision=HIGHEST, preferred_element_type=f32)
    for level in (2, 1, 0):
        before, source, gain = [ref[...] for ref in posts[3 * level : 3 * level + 3]]
        field = before + double_rows(field, scratch)
        stiffness = 0.25**level
        constant = gain * source
        gain = gain * stiffness
        for sweep in range(2):
            field = (1.0 - damping) * field + constant + gain * around(field, 2**level)
        if level > 0:
            field = field[4 : field.shape[0] - 4]
    out_ref[...] = field[8 : 8 + height, :width]


def swap_pairs(counts, axis):
    nx, ny = counts
    even, odd = [], []
    for i in range(nx):
        for j in range(ny):
            here = i * ny + j
            place = (i, j)[axis]
            last = counts[axis] - 1
            hop = ny if axis == 0 else 1
            even.append((here, here + hop * (1 - 2 * (place % 2))))
            if place in (0, last):
                other = ((last - i) * ny + j) if axis == 0 else ((i ^ 1) * ny + j)
                odd.append((here, other))
            else:
                odd.append((here, here + hop * (2 * (place % 2) - 1)))
    return even, odd


def params():
    return pltpu.CompilerParams(vmem_limit_bytes=VMEM_BYTES)


def shape(*dims):
    return jax.ShapeDtypeStruct(dims, f32)


def per_device(counts, right_side, kappa_field, ice_blocks):
    height, width = right_side.shape
    grid_rows, grid_cols = height * counts[0], width * counts[1]
    axes = ("gx", "gy")
    right_side, kappa_field, ice_blocks = [
        pltpu.with_memory_space_constraint(x, pltpu.HBM) for x in (right_side, kappa_field, ice_blocks)
    ]
    row_even, row_odd = swap_pairs(counts, 0)
    col_even, col_odd = swap_pairs(counts, 1)
    packed = 2 * (height + height * FAR // LANES)
    right_side, reaction, even, odd, odd_rows = pl.pallas_call(
        edges_kernel,
        out_shape=(
            shape(height, width),
            shape(height, width),
            shape(packed, LANES),
            shape(packed, LANES),
            shape(2 * ROWS, width),
        ),
        in_specs=[pl.BlockSpec(memory_space=pltpu.HBM)] * 3,
        scratch_shapes=[
            pltpu.VMEM((height, width), f32),
            pltpu.VMEM(ice_blocks.shape, jnp.int32),
            pltpu.SemaphoreType.DMA((3,)),
        ],
        compiler_params=params(),
        name="edges",
    )(right_side, kappa_field, ice_blocks)
    odd_rows = lax.ppermute(odd_rows, axes, row_odd)
    odd = lax.ppermute(odd, axes, col_odd)
    even = lax.ppermute(even, axes, col_even)
    total = width + 2 * NEAR + LANES
    even_rows, odd_corners = pl.pallas_call(
        rows_kernel,
        out_shape=(shape(2 * ROWS, total), shape(ROWS, 5 * LANES)),
        compiler_params=params(),
        name="rows",
    )(right_side, reaction, even, odd, odd_rows)
    odd_corners = lax.ppermute(odd_corners, axes, row_odd)
    even_rows = lax.ppermute(even_rows, axes, row_even)
    half = height // 8
    post_shapes = []
    for level in range(3):
        post_shapes += [shape((height >> level) + 16, width + LANES)] * 3
    coarse_rows = half + ROWS // 4
    outs = pl.pallas_call(
        functools.partial(down_kernel, height, width, grid_rows, grid_cols),
        out_shape=(*post_shapes, shape(2 * coarse_rows, LANES), shape(2 * half, LANES), shape(2 * half, LANES)),
        scratch_shapes=[pltpu.VMEM((total // LANES, height + 2 * ROWS, LANES), f32)],
        compiler_params=params(),
        name="down",
    )(right_side, reaction, even, odd, even_rows, odd_rows, odd_corners)
    posts, own, even, odd = outs[:9], outs[9], outs[10], outs[11]
    odd = lax.ppermute(odd, axes, row_odd)
    even = lax.ppermute(even, axes, row_even)
    return pl.pallas_call(
        functools.partial(up_kernel, height, width, grid_rows, grid_cols),
        out_shape=shape(height, width),
        scratch_shapes=[
            pltpu.VMEM((width // LANES + 1, height + 16, LANES), f32),
            pltpu.VMEM((2, half * 3 + 16, LANES), f32),
        ],
        compiler_params=params(),
        name="up",
    )(*posts, own, even, odd)


def solution(mesh):
    counts = (mesh.shape["gx"], mesh.shape["gy"])
    return jax.shard_map(
        functools.partial(per_device, counts),
        mesh=mesh,
        in_specs=(P("gx", "gy"),) * 3,
        out_specs=P("gx", "gy"),
        check_vma=False,
    )
```

```python
import functools

import jax
import jax.numpy as jnp
from jax import lax
from jax.experimental import pallas as pl
from jax.experimental.pallas import tpu as pltpu
from jax.sharding import PartitionSpec as P

BLOCK = 8
NC = 16
LANES = 128
ROWS = 32
NEAR = 128
FAR = 32
VMEM_BYTES = 12 * 2**20
damping = 0.8

f32 = jnp.float32
bf16 = jnp.bfloat16


def roll(value, shift, axis):
    return pltpu.roll(value, shift % value.shape[axis], axis)


def around(value, step):
    rows = roll(value, 1, 0) + roll(value, -1, 0)
    return rows + (roll(value, step, 1) + roll(value, -step, 1))


def iota(shape, axis):
    return lax.broadcasted_iota(jnp.int32, shape, axis)


def ones_where(condition):
    return jnp.where(condition, 1.0, 0.0).astype(f32)


def pack_near_far(tiles, near_tile, far_tile, far_lane):
    far = tiles[:, far_tile * LANES : (far_tile + 1) * LANES]
    near = tiles[:, near_tile * LANES : (near_tile + 1) * LANES]
    count = LANES // FAR
    group = tiles.shape[0] // count
    lane = iota((group, LANES), 1) // FAR
    packed = jnp.zeros((group, LANES), f32)
    for g in range(count):
        moved = roll(far[g * group : (g + 1) * group], FAR * g - far_lane, 1)
        packed = jnp.where(lane == g, moved, packed)
    return near, packed


def edges_kernel(*refs):
    ins, right_ref, reaction_ref, even_ref, odd_ref, rows_ref = refs[:3], *refs[3:8]
    kappa_ref, ice_ref, sems = refs[8:11]
    copies = []
    for k, (src, dst) in enumerate(zip(ins, (right_ref, kappa_ref, ice_ref))):
        copies.append(pltpu.make_async_copy(src, dst, sems.at[k]))
    for copy in copies:
        copy.start()
    height, width = right_ref.shape
    blocks = ice_ref.shape
    spread = ones_where(iota((blocks[1], width), 1) // BLOCK == iota((blocks[1], width), 0))
    repeat = ones_where(iota((height, blocks[0]), 0) // BLOCK == iota((height, blocks[0]), 1))
    for copy in copies:
        copy.wait()
    ice = ice_ref[...].astype(f32)
    ice = jnp.dot(ice, spread, preferred_element_type=f32)
    ice = jnp.dot(repeat, ice, preferred_element_type=f32)
    reaction = kappa_ref[...] * (1.0 + 3.0 * (1.0 - ice))
    reaction_ref[...] = reaction
    tiles = width // LANES
    even = lax.rem(lax.axis_index("gy"), 2) == 0
    even_row = lax.rem(lax.axis_index("gx"), 2) == 0
    size = height + height * FAR // LANES
    for k, field in enumerate((right_ref[...], reaction)):
        to_right = pack_near_far(field, tiles - 1, tiles - 2, LANES - FAR)
        to_left = pack_near_far(field, 0, 1, 0)
        start = k * size
        for a, b in zip(to_right, to_left):
            stop = start + a.shape[0]
            even_ref[start:stop, :] = jnp.where(even, a, b)
            odd_ref[start:stop, :] = jnp.where(even, b, a)
            start = stop
        edge = jnp.where(even_row, field[:ROWS], field[height - ROWS :])
        for j in range(tiles):
            rows_ref[k * tiles + j] = edge[:, j * LANES : (j + 1) * LANES]


def exact_dot(value, table):
    rows = value.shape[0]
    parts = []
    for _ in range(3):
        part = value.astype(bf16)
        parts.append(part)
        value = value - part.astype(f32)
    out = jnp.dot(jnp.concatenate(parts, axis=0), table.astype(bf16), preferred_element_type=f32)
    return out[:rows] + out[rows : 2 * rows] + out[2 * rows :]


def own_tile(own_ref, even_ref, odd_ref, even, k, j, start, count):
    height, width = own_ref.shape
    tiles = width // LANES
    size = even_ref.shape[0] // 2
    if 1 <= j <= tiles:
        return own_ref[start : start + count, (j - 1) * LANES : j * LANES]
    if j <= tiles + 1:
        rows = pl.ds(k * size + start, count)
        first, second = even_ref[rows, :], odd_ref[rows, :]
        return jnp.where(even, first, second) if j else jnp.where(even, second, first)
    group = height * FAR // LANES
    g = start // group
    rows = pl.ds(k * size + height + start % group, count)
    first, second = even_ref[rows, :], odd_ref[rows, :]
    lane = iota((count, LANES), 1)
    right = roll(jnp.where(even, first, second), -FAR * g, 1)
    left = roll(jnp.where(even, second, first), LANES - FAR - FAR * g, 1)
    return jnp.where(lane < FAR, right, jnp.where(lane >= LANES - FAR, left, 0.0))


def rows_kernel(right_ref, reaction_ref, even_ref, odd_ref, unread_ref, even_out, odd_out):
    height, width = right_ref.shape
    tiles = width // LANES
    even_column = lax.rem(lax.axis_index("gy"), 2) == 0
    even_row = lax.rem(lax.axis_index("gx"), 2) == 0
    far = []
    for k, ref in enumerate((right_ref, reaction_ref)):
        for j in range(tiles + 3):
            up = own_tile(ref, even_ref, odd_ref, even_column, k, j, 0, ROWS)
            down = own_tile(ref, even_ref, odd_ref, even_column, k, j, height - ROWS, ROWS)
            even_out[k * (tiles + 3) + j] = jnp.where(even_row, down, up)
            odd = jnp.where(even_row, up, down)
            if j in (0, tiles + 1):
                odd_out[2 * k + (j > 0)] = odd
            elif j > tiles:
                far.append(odd)
    lane = iota((ROWS, LANES), 1)
    odd_out[4] = jnp.where((lane >= FAR) & (lane < LANES - FAR), roll(far[1], LANES // 2, 1), far[0])


def beside(tiles, step):
    lane = iota(tiles[0].shape, 1)
    forward = [roll(t, step, 1) for t in tiles]
    backward = [roll(t, -step, 1) for t in tiles]
    count = len(tiles)
    return [
        jnp.where(lane < step, forward[j - 1], forward[j])
        + jnp.where(lane >= LANES - step, backward[(j + 1) % count], backward[j])
        for j in range(count)
    ]


def around_strip(ref, row, step):
    count = ref.shape[0]
    here = [ref[j, row : row + 8] for j in range(count)]
    side = beside(here, step)
    total = [(ref[j, row - 1 : row + 7] + ref[j, row + 1 : row + 9]) + side[j] for j in range(count)]
    return here, total


def down_kernel(counts, *refs):
    right_ref, reaction_ref, even_ref, odd_ref, even_rows, odd_rows, odd_corners = refs[:7]
    starts, fields, gains = refs[7:10], refs[10:13], refs[13:16]
    own_out, even_out, odd_out = refs[16:19]
    sources, reactions, residuals = refs[19:22], refs[22:25], refs[25:28]
    height, width = right_ref.shape
    tiles = width // LANES
    count = tiles + 3
    gx, gy = lax.axis_index("gx"), lax.axis_index("gy")
    even_column = lax.rem(gy, 2) == 0
    even_row = lax.rem(gx, 2) == 0
    zero = jnp.zeros((8, LANES), f32)
    lane = iota((8, LANES), 1)
    top_in = jnp.where(gx > 0, 1.0, 0.0).astype(f32)
    bottom_in = jnp.where(gx < counts[0] - 1, 1.0, 0.0).astype(f32)
    left_in = jnp.where(gy > 0, damping, 0.0).astype(f32)
    right_in = jnp.where(gy < counts[1] - 1, damping, 0.0).astype(f32)
    scale = [jnp.full((8, LANES), damping, f32)] * count
    scale[0] = jnp.full((8, LANES), left_in, f32)
    scale[tiles + 1] = jnp.full((8, LANES), right_in, f32)
    scale[tiles + 2] = jnp.where(lane < FAR, right_in, jnp.where(lane >= LANES - FAR, left_in, 0.0))

    def first_tile(k, j, row):
        own = (right_ref, reaction_ref)[k]
        if ROWS <= row < ROWS + height:
            return own_tile(own, even_ref, odd_ref, even_column, k, j, row - ROWS, 8)
        top = row < ROWS
        row = row if top else row - ROWS - height
        if 1 <= j <= tiles:
            odd = odd_rows[k * tiles + j - 1, row : row + 8]
        elif j <= tiles + 1:
            odd = odd_corners[2 * k + (j > 0), row : row + 8]
        else:
            odd = odd_corners[4, row : row + 8]
            odd = roll(odd, LANES // 2, 1) if k else odd
        even = even_rows[k * count + j, row : row + 8]
        return jnp.where(even_row, odd, even) if top else jnp.where(even_row, even, odd)

    def paired(ref, row, step, lanes=True):
        pairs = [
            ref[j, pl.ds(2 * row + 8, 8, stride=2), :] + ref[j, pl.ds(2 * row + 9, 8, stride=2), :]
            for j in range(count)
        ]
        if not lanes:
            return pairs
        moved = [roll(t, -step, 1) for t in pairs]
        return [
            0.25 * (pairs[j] + jnp.where(lane >= LANES - step, moved[(j + 1) % count], moved[j]))
            for j in range(count)
        ]

    margin = ROWS
    for level in range(3):
        rows = (height >> level) + 2 * margin
        stiffness = 0.25**level
        step = 2**level
        start, field, gain = starts[level], fields[level], gains[level]
        source, reaction, residual = sources[level], reactions[level], residuals[level]
        for ref in (start, field):
            for j in range(count):
                ref[j, :8] = zero
                ref[j, rows + 8 :] = zero
        for row in range(0, rows, 8):
            if level == 0:
                pieces = [[first_tile(k, j, row) for j in range(count)] for k in range(2)]
            else:
                pieces = [
                    paired(ref[level - 1], row, step // 2) for ref in (residuals, reactions)
                ]
            for j in range(count):
                value = scale[j] / (pieces[1][j] + 4.0 * stiffness)
                if row < margin:
                    value = value * top_in
                elif row >= rows - margin:
                    value = value * bottom_in
                place = pl.ds(row + 8, 8)
                source[j, place] = pieces[0][j]
                reaction[j, place] = pieces[1][j]
                start[j, place] = value * pieces[0][j]
                gain[j, place] = value * stiffness if level else value
        for row in range(8, rows + 8, 8):
            here, total = around_strip(start, row, step)
            for j in range(count):
                field[j, row : row + 8] = (2.0 - damping) * here[j] + gain[j, row : row + 8] * total[j]
        for row in range(8, rows + 8, 8):
            here, total = around_strip(field, row, step)
            for j in range(count):
                place = pl.ds(row, 8)
                diagonal = reaction[j, place] + 4.0 * stiffness
                near = stiffness * total[j] if level else total[j]
                residual[j, place] = (source[j, place] - diagonal * here[j]) + near
        margin //= 2
    total = count * LANES
    cell = iota((total, LANES), 0)
    step = 4
    target = jnp.where(cell >= total - FAR, cell - total + 8 * LANES, cell) // 8
    valid = (cell % step == 0) & ((cell < total - LANES + FAR) | (cell >= total - FAR))
    gather = ones_where(valid & (target == iota((total, LANES), 1)))
    coarse_rows = height // 8 + 2 * margin
    strips = []
    for ref in (residuals[2], reactions[2]):
        for row in range(0, coarse_rows, 8):
            strips.append(jnp.concatenate(paired(ref, row, step, lanes=False), axis=1))
    compact = 0.25 * exact_dot(jnp.concatenate(strips, axis=0), gather)
    own_out[...] = compact
    half = height // 8
    for k in range(2):
        base = k * coarse_rows + margin
        to_next = compact[base - 1 : base - 1 + half]
        to_last = compact[base + 1 : base + 1 + half]
        even_out[k * half : (k + 1) * half] = jnp.where(even_row, to_next, to_last)
        odd_out[k * half : (k + 1) * half] = jnp.where(even_row, to_last, to_next)


def up_kernel(counts, *refs):
    starts, befores, gains = refs[:3], refs[3:6], refs[6:9]
    own_ref, even_ref, odd_ref = refs[9:12]
    out_ref = refs[12]
    region = refs[13]
    firsts, seconds = refs[14:17], refs[17:20]
    buffer, sems = refs[20:22]
    height, width = out_ref.shape
    tiles = width // LANES
    gx, gy = lax.axis_index("gx"), lax.axis_index("gy")
    even_row = lax.rem(gx, 2) == 0
    half = height // 8
    coarse_rows = own_ref.shape[0] // 2
    margin = (coarse_rows - half) // 2
    lead = 8 + half
    rows = region.shape[1]
    region[...] = jnp.zeros_like(region)
    for k in range(2):
        a = even_ref[k * half : (k + 1) * half]
        b = odd_ref[k * half : (k + 1) * half]
        own = own_ref[k * coarse_rows : (k + 1) * coarse_rows]
        region[k, lead - 1 - half : lead - 1] = jnp.where(even_row, b, a)
        region[k, lead - 1 : lead + half + 1] = own[margin - 1 : margin + half + 1]
        region[k, lead + half + 1 : lead + 2 * half + 1] = jnp.where(even_row, a, b)
    stiffness = 0.25**3
    row = gx * half - lead + iota((rows, LANES), 0)
    col = iota((rows, LANES), 1)
    col = jnp.where(col >= LANES - FAR // 8, col - LANES, col) - NEAR // 8
    col = col + gy * (width // 8)
    inside = (row >= 0) & (row < counts[0] * half) & (col >= 0) & (col < counts[1] * (width // 8))
    gain = ones_where(inside) * (damping / (region[1] + 4.0 * stiffness))
    field = gain * region[0]
    constant = field
    gain = gain * stiffness
    for sweep in range(NC - 1):
        field = (1.0 - damping) * field + constant + gain * around(field, 1)
    field = field[lead - margin : lead - margin + coarse_rows]
    total = width + LANES
    position = iota((LANES, total), 1)
    position = jnp.where(position >= width + LANES // 2, position - total, position)
    expand = ones_where((position + NEAR) // 8 == iota((LANES, total), 0))
    field = exact_dot(field, expand)
    lane = iota((8, LANES), 1)
    zero = jnp.zeros((8, LANES), f32)

    def tile_of(ref, j, place):
        if j < tiles:
            return ref[j + 1, place, :]
        return jnp.where(lane < LANES // 2, ref[tiles + 1, place, :], ref[0, place, :])

    def begin(level, row, pieces):
        shift = (befores[level].shape[1] - firsts[level].shape[1]) // 2
        for j, piece in enumerate(pieces):
            for odd in range(2):
                place = pl.ds(2 * row + 8 - shift + odd, 8, stride=2)
                from_place = pl.ds(2 * row + 8 + odd, 8, stride=2)
                firsts[level][j, place, :] = tile_of(befores[level], j, from_place) + piece

    def sweep_strip(ref, level, row, count):
        base = (starts[level].shape[1] - ref.shape[1]) // 2
        here, total = around_strip(ref, row, 2**level)
        place = pl.ds(row + base, 8)
        return [
            ((1.0 - damping) * here[j] + tile_of(starts[level], j, place))
            + tile_of(gains[level], j, place) * total[j]
            for j in range(count)
        ]

    for row in range(0, coarse_rows, 8):
        begin(2, row, [field[row : row + 8, j * LANES : (j + 1) * LANES] for j in range(tiles + 1)])
    for level in (2, 1, 0):
        first, second = firsts[level], seconds[level]
        rows = first.shape[1] - 16
        step = 2**level
        skip = 8 if level < 2 else 0
        for j in range(tiles + 1):
            for ref in (first, second) if level == 2 else (second,):
                ref[j, skip : skip + 8] = zero
                ref[j, rows + 8 - skip : rows + 16 - skip] = zero
        for row in range(8 + skip, rows + 8 - skip, 8):
            pieces = sweep_strip(first, level, row, tiles + 1)
            for j in range(tiles + 1):
                second[j, row : row + 8] = pieces[j]
        if level > 0:
            bit = step // 2
            for row in range(8 + skip, rows + 8 - skip, 8):
                pieces = sweep_strip(second, level, row, tiles + 1)
                moved = [roll(t, bit, 1) for t in pieces]
                pieces = [
                    jnp.where(
                        (lane // bit) % 2 == 1,
                        jnp.where(lane < bit, moved[j - 1], moved[j]),
                        pieces[j],
                    )
                    for j in range(tiles + 1)
                ]
                begin(level - 1, row - 8, pieces)
        else:
            chunk = height // sems.shape[0]
            copies = []
            for row in range(0, height, 8):
                pieces = sweep_strip(second, level, row + 8 + (rows - height) // 2, tiles)
                for j in range(tiles):
                    buffer[row : row + 8, j * LANES : (j + 1) * LANES] = pieces[j]
                if (row + 8) % chunk == 0:
                    place = pl.ds(row + 8 - chunk, chunk)
                    copy = pltpu.make_async_copy(buffer.at[place], out_ref.at[place], sems.at[row // chunk])
                    copy.start()
                    copies.append(copy)
            for copy in copies:
                copy.wait()


def swap_pairs(counts, axis):
    nx, ny = counts
    even, odd = [], []
    for i in range(nx):
        for j in range(ny):
            here = i * ny + j
            place = (i, j)[axis]
            last = counts[axis] - 1
            hop = ny if axis == 0 else 1
            even.append((here, here + hop * (1 - 2 * (place % 2))))
            if place in (0, last):
                other = ((last - i) * ny + j) if axis == 0 else ((i ^ 1) * ny + j)
                odd.append((here, other))
            else:
                odd.append((here, here + hop * (2 * (place % 2) - 1)))
    return even, odd


def params():
    return pltpu.CompilerParams(vmem_limit_bytes=VMEM_BYTES)


def shape(*dims):
    return jax.ShapeDtypeStruct(dims, f32)


def per_device(counts, right_side, kappa_field, ice_blocks):
    height, width = right_side.shape
    tiles = width // LANES
    count = tiles + 3
    axes = ("gx", "gy")
    right_side, kappa_field, ice_blocks = [
        pltpu.with_memory_space_constraint(x, pltpu.HBM) for x in (right_side, kappa_field, ice_blocks)
    ]
    row_even, row_odd = swap_pairs(counts, 0)
    col_even, col_odd = swap_pairs(counts, 1)
    packed = 2 * (height + height * FAR // LANES)
    right_side, reaction, even, odd, odd_rows = pl.pallas_call(
        edges_kernel,
        out_shape=(
            shape(height, width),
            shape(height, width),
            shape(packed, LANES),
            shape(packed, LANES),
            shape(2 * tiles, ROWS, LANES),
        ),
        in_specs=[pl.BlockSpec(memory_space=pltpu.HBM)] * 3,
        scratch_shapes=[
            pltpu.VMEM((height, width), f32),
            pltpu.VMEM(ice_blocks.shape, jnp.int32),
            pltpu.SemaphoreType.DMA((3,)),
        ],
        compiler_params=params(),
        name="edges",
    )(right_side, kappa_field, ice_blocks)
    odd_rows = lax.ppermute(odd_rows, axes, row_odd)
    odd = lax.ppermute(odd, axes, col_odd)
    even = lax.ppermute(even, axes, col_even)
    even_rows, odd_corners = pl.pallas_call(
        rows_kernel,
        out_shape=(shape(2 * count, ROWS, LANES), shape(5, ROWS, LANES)),
        compiler_params=params(),
        name="rows",
    )(right_side, reaction, even, odd, odd_rows)
    odd_corners = lax.ppermute(odd_corners, axes, row_odd)
    even_rows = lax.ppermute(even_rows, axes, row_even)
    half = height // 8
    levels = [(count, ((height + 2 * ROWS) >> level) + 16, LANES) for level in range(3)]
    coarse_rows = half + ROWS // 4
    outs = pl.pallas_call(
        functools.partial(down_kernel, counts),
        out_shape=(
            *[shape(*dims) for dims in levels * 3],
            shape(2 * coarse_rows, LANES),
            shape(2 * half, LANES),
            shape(2 * half, LANES),
        ),
        scratch_shapes=[pltpu.VMEM(dims, f32) for dims in levels * 3],
        compiler_params=params(),
        name="down",
    )(right_side, reaction, even, odd, even_rows, odd_rows, odd_corners)
    posts, own, even, odd = outs[:9], outs[9], outs[10], outs[11]
    odd = lax.ppermute(odd, axes, row_odd)
    even = lax.ppermute(even, axes, row_even)
    fields = [(tiles + 1, (height >> level) + 2 * (16 if level < 2 else 8) + 16, LANES) for level in range(3)]
    return pl.pallas_call(
        functools.partial(up_kernel, counts),
        out_shape=shape(height, width),
        out_specs=pl.BlockSpec(memory_space=pltpu.HBM),
        scratch_shapes=[
            pltpu.VMEM((2, half * 3 + 16, LANES), f32),
            *[pltpu.VMEM(dims, f32) for dims in fields * 2],
            pltpu.VMEM((height, width), f32),
            pltpu.SemaphoreType.DMA((4,)),
        ],
        compiler_params=params(),
        name="up",
    )(*posts, own, even, odd)


def solution(mesh):
    counts = (mesh.shape["gx"], mesh.shape["gy"])
    return jax.shard_map(
        functools.partial(per_device, counts),
        mesh=mesh,
        in_specs=(P("gx", "gy"),) * 3,
        out_specs=P("gx", "gy"),
        check_vma=False,
    )
```
